32 devices in a mesh: row: 4 (over z), col: 4 (over y, core), rep: 2 (over x).
Axes of the slice: x: 2, y: 2, z: 4, core: 2. Of those that a mesh axis runs over, the one named last changes fastest.
Arguments:
- upstream: float32 [16384, 16384], P('row', ('col', 'rep')), may hold values from -0.046875 to 0.046875
- input_panel: float32 [16384, 1024], P('row', ('col', 'rep')), may hold values from -6 to 6
Outputs:
- panel_grad: float32 [16384, 1024], P('row', ('col', 'rep'))
The draws below stay inside these ranges and needn't reach their ends.
All inputs are finite; a program needn't handle non-finite values.
Results may differ from the reference program's by a relative error of at most 0.000071.
Values sent between devices are 32-bit elements; how exact they have to be, the bound alone decides.
A program may use at most 192 MiB of HBM per device.

```python
import jax
import jax.numpy as jnp
from jax import lax

N = 16384
K = 1024


def block_scale(stream_key, extent, split, least, high):
    def one(dim, parts):
        draws = jax.random.uniform(jax.random.fold_in(jax.random.fold_in(stream_key, 6), dim), (parts,), jnp.float32, least / len(split), high / len(split))
        return jnp.repeat(jnp.exp(draws), extent[dim] // parts).reshape((-1,) + (1,) * (len(extent) - dim - 1))

    level = one(*split[0])
    for cut in split[1:]:
        level = level * one(*cut)
    return level


def scatter_about(key, extent, scale, bound, shards=(), dtype=jnp.bfloat16):
    level = block_scale(key, extent, shards, -0.22, 0.18) if shards else 1.0
    array = jax.random.normal(key, extent, jnp.float32) * scale * level
    return jnp.minimum(jnp.maximum(array, -bound), bound).astype(dtype)


def setup_inputs(seed: int = 0) -> dict:
    streams_of = jax.random.split(jax.random.key(seed), 3)
    upstream = scatter_about(streams_of[0], (N, N), N ** -0.5, 0.046875, ((0, 4), (1, 8)), jnp.float32)
    input_panel = scatter_about(streams_of[1], (N, K), 1.0, 6.0, ((0, 4), (1, 8)), jnp.float32)
    return {"upstream": upstream, "input_panel": input_panel}


def reference(upstream, input_panel):
    precise = lax.Precision.HIGHEST
    lower_tile = jnp.tril(upstream)
    direct = jnp.dot(lower_tile, input_panel, precision=precise, preferred_element_type=jnp.float32)
    mirror = lax.dot_general(lower_tile, input_panel, (((0,), (0,)), ((), ())), precision=precise, preferred_element_type=jnp.float32)
    return direct + mirror
```

```python
import jax
import jax.numpy as jnp
from jax import lax
from jax.sharding import PartitionSpec as P

GROUP = ("col", "rep")


def product(left, right, contract):
    return lax.dot_general(
        left,
        right,
        (contract, ((), ())),
        precision=lax.Precision.HIGH,
        preferred_element_type=jnp.float32,
    )


def after(value, *first):
    return lax.optimization_barrier((value,) + first)[0]


def rows_up(own, rows):
    me = lax.axis_index("row")
    gathered = jnp.zeros((rows,) + own.shape, own.dtype)
    held = early = own
    for step in range(rows):
        slot = lax.rem(me + rows - step, rows)
        gathered = lax.dynamic_update_slice_in_dim(gathered, held[None], slot, 0)
        if step < rows - 1:
            held = lax.ppermute(held, "row", [(r, r + 1) for r in range(step, rows - 1)])
            if step < rows - 2:
                early = held
    return gathered, early


def rows_down(parts, rows):
    me = lax.axis_index("row")
    arrived = None
    for step in range(1, rows):
        block = jnp.maximum(me + step - rows, 0)
        term = lax.dynamic_index_in_dim(parts, block, 0, keepdims=False)
        total = term if arrived is None else term + arrived
        arrived = lax.ppermute(total, "row", [(r, r - 1) for r in range(rows - step, rows)])
        if step == 1:
            first = arrived
    own = lax.dynamic_index_in_dim(parts, me, 0, keepdims=False)
    if arrived is None:
        return own, own
    return own + arrived, first


def per_device(rows, groups, upstream, input_panel):
    row_count, col_count = upstream.shape
    width = input_panel.shape[1]
    ratio = row_count // col_count
    row_index = lax.axis_index("row")
    col_index = lax.axis_index(GROUP)
    rows_global = row_index * row_count + lax.broadcasted_iota(jnp.int32, (row_count, col_count), 0)
    cols_global = col_index * col_count + lax.broadcasted_iota(jnp.int32, (row_count, col_count), 1)
    lower_tile = jnp.where(cols_global <= rows_global, upstream, jnp.float32(0.0))

    panel_t = jnp.transpose(input_panel)
    band_t = lax.all_gather(panel_t, GROUP, axis=0, tiled=True)
    pieces = jnp.transpose(input_panel.reshape(ratio, col_count, width), (0, 2, 1))
    column_blocks, early = rows_up(pieces, rows)
    column_blocks = column_blocks.reshape(groups, width, col_count)

    upper_t = product(after(band_t, early), lower_tile, ((1,), (0,)))
    upper_blocks = lax.all_to_all(
        upper_t.reshape(groups, width, col_count), GROUP, split_axis=0, concat_axis=0, tiled=True
    )
    upper_total, first = rows_down(upper_blocks.reshape(rows, ratio, width, col_count), rows)

    column_t = lax.all_to_all(
        after(column_blocks, upper_blocks), GROUP, split_axis=0, concat_axis=0, tiled=True
    )
    lower_t = product(after(column_t, first).reshape(groups * width, col_count), lower_tile, ((1,), (1,)))
    lower_total = lax.psum_scatter(lower_t, GROUP, scatter_dimension=0, tiled=True)

    upper_rows = jnp.transpose(upper_total, (0, 2, 1)).reshape(row_count, width)
    return upper_rows + jnp.transpose(lower_total)


def solution(mesh):
    rows = mesh.shape["row"]
    groups = mesh.shape["col"] * mesh.shape["rep"]
    placed = P("row", GROUP)

    def body(upstream, input_panel):
        return per_device(rows, groups, upstream, input_panel)

    return jax.shard_map(
        body, mesh=mesh, in_specs=(placed, placed), out_specs=placed, check_vma=False
    )
```
